512 devices in a mesh: row: 32 (over x_lo, z), col: 16 (over y, x_hi, core).
Axes of the slice: x: 4 (x_hi: 2, x_lo: 2; x = x_hi * 2 + x_lo), y: 4, z: 16, core: 2. Of those that a mesh axis runs over, the one named last changes fastest.
Arguments:
- gradient: bfloat16 [8192, 28672], P('row', 'col'), may hold values from -6 to 6
- projector: bfloat16 [8192, 1024], P('row'), may hold values from -0.375 to 0.375
- first_moment: float32 [1024, 28672], P('row', 'col'), may hold values from -6 to 6
- second_moment: float32 [1024, 28672], P('row', 'col'), may hold values from 5e-05 to 0.12, as said below
Outputs:
- update: bfloat16 [8192, 28672], P('row', 'col')
- first_new: float32 [1024, 28672], P('row', 'col')
- second_new: float32 [1024, 28672], P('row', 'col')
The draws below stay inside these ranges and needn't reach their ends.
Inputs may be any that keep to these rules, and one draw needn't show every extreme that they name: `second_moment`: entries are positive.
All inputs are finite; a program needn't handle non-finite values.
Results may differ from the reference program's by a relative error of at most 0.038.
Values may be sent and summed in bfloat16 or wider, within the bound.
No kernel may reach another device: no remote copies, remote signals or barrier semaphores. Data moves between devices by JAX's collectives and lax.ppermute only.
A program may use at most 64 MiB of HBM per device.

```python
import math
import jax
import jax.numpy as jnp
from jax import lax

D = 8192
FF = 28672
R = 1024
N_ROW = 32


def draw_second_moment(key, part):
    key_base = jax.random.fold_in(key, 11)
    key_column = jax.random.fold_in(key, 12)
    position = jnp.arange(R, dtype=jnp.float32)[:, None] / R
    column_place = jnp.arange(FF, dtype=jnp.float32)[None, :] / FF
    column_noise = jax.random.uniform(key_column, (1, FF), jnp.float32, 0.0, 1.0)
    base = jax.random.uniform(key_base, (R, FF), jnp.float32, 0.5, 2.0)
    return 0.0001 * base * jnp.exp(math.log(10.0) * (position + 0.5 * column_place + 0.5 * column_noise))


def spiked(entries, key, source, target, parts, factor):
    def block_of(axis_at):
        return (jnp.arange(entries.shape[axis_at]) // (entries.shape[axis_at] // parts)).reshape((-1,) + (1,) * (entries.ndim - 1 - axis_at))

    first = jax.random.permutation(key, parts)[block_of(target)]
    second = (block_of(target) + parts // 2) % parts
    return jnp.where((block_of(source) == first) | (block_of(source) == second), factor * entries, entries)


def levels(stream_key, extent, pieces, least, largest):
    factor_of, own = 1.0, jax.random.fold_in(stream_key, 6)
    for dim, parts in pieces:
        heights = jnp.exp(jax.random.uniform(jax.random.fold_in(own, dim), (parts,), jnp.float32, least / len(pieces), largest / len(pieces)))
        factor_of = factor_of * jnp.repeat(heights, extent[dim] // parts).reshape([-1 if axis == dim else 1 for axis in range(len(extent))])
    return factor_of


def gaussian(own_key, extent, spread, limit, split=(), held_as=jnp.bfloat16):
    factor_of = levels(own_key, extent, split, -0.22, 0.18) if split else 1.0
    drawn = jax.random.normal(own_key, extent, jnp.float32) * spread * factor_of
    return jnp.minimum(jnp.maximum(drawn, -limit), limit).astype(held_as)


def bell_draw_with(stream_key, extent, spread, bound, shards, heavy, kind=jnp.bfloat16):
    drawn = spread * jax.random.normal(stream_key, extent, jnp.float32)
    if shards:
        drawn = drawn * levels(stream_key, extent, shards, -0.22, 0.18)
    return jnp.clip(spiked(drawn, jax.random.fold_in(stream_key, 3), *heavy), -bound, bound).astype(kind)


def setup_inputs(seed: int = 0) -> dict:
    key_list = jax.random.split(jax.random.key(seed), 5)
    return {
        "gradient": gaussian(key_list[0], (D, FF), 1.0, 6.0, ((0, 32), (1, 16))),
        "projector": bell_draw_with(key_list[1], (D, R), R ** -0.5, 0.375, ((0, 32),), (0, 1, 32, 2.75)),
        "first_moment": gaussian(key_list[2], (R, FF), 1.0, 6.0, ((0, 32), (1, 16)), jnp.float32),
        "second_moment": draw_second_moment(jax.random.fold_in(key_list[4], 71), 0),
    }


decay_first = 0.9
decay_second = 0.999
bias_first = 1.0 - 0.9 ** 10
bias_second = 1.0 - 0.999 ** 10
epsilon = 1e-08
clip_limit = 0.5

def reference(gradient, projector, first_moment, second_moment):
    block_rows = D // N_ROW

    def block_term(index, running):
        offset = (index * block_rows).astype(jnp.int32)
        basis_block = lax.dynamic_slice_in_dim(projector, offset, block_rows, 0)
        grad_block = lax.dynamic_slice_in_dim(gradient, offset, block_rows, 0)
        product = lax.dot_general(basis_block, grad_block, (((0,), (0,)), ((), ())), preferred_element_type=jnp.float32)
        rounded = lax.optimization_barrier(product.astype(jnp.bfloat16))
        return running + rounded.astype(jnp.float32)
    lowrank = lax.fori_loop(0, N_ROW, block_term, jnp.zeros((R, FF), jnp.float32))
    first_new = decay_first * first_moment + (1.0 - decay_first) * lowrank
    second_new = decay_second * second_moment + (1.0 - decay_second) * lowrank * lowrank
    direction = first_new / bias_first / (jnp.sqrt(second_new / bias_second) + epsilon)
    root_mean = jnp.sqrt(jnp.sum(direction * direction) / (R * FF) + 1e-06)
    factor = jnp.minimum(1.0, clip_limit / root_mean)
    step_low = (factor * direction).astype(jnp.bfloat16)
    update = jnp.dot(projector, step_low, preferred_element_type=jnp.float32).astype(jnp.bfloat16)
    return (update, first_new, second_new)
```

```python
import functools

import jax
import jax.numpy as jnp
from jax import lax
from jax.sharding import Mesh
from jax.sharding import PartitionSpec as P

FF = 28672
R = 1024
ROW = ("row_0", "row_1")
ROW_COL = ("row_0", "row_1", "col_0", "col_1", "col_2")
COL = ("col_0", "col_1", "col_2")


decay_first = 0.9
decay_second = 0.999
bias_first = 1.0 - 0.9**10
bias_second = 1.0 - 0.999**10
epsilon = 1e-08
clip_limit = 0.5


def by_axis(shard, axes):
    return functools.reduce(lax.psum, axes, shard)


def exchanged(pieces, axis):
    return lax.all_to_all(pieces, axis, split_axis=0, concat_axis=0, tiled=True)


def local(gradient, projector, first_moment, second_moment):
    row_0, row_1 = (lax.axis_size(a) for a in ROW)
    rows = first_moment.shape[0]
    product = lax.dot_general(
        projector, gradient, (((0,), (0,)), ((), ())), preferred_element_type=jnp.float32
    )
    pieces = product.astype(jnp.bfloat16).reshape(row_0, row_1, rows, -1).swapaxes(0, 1)
    pieces = lax.psum_scatter(
        pieces.reshape(row_1 * row_0, rows, -1), "row_1", scatter_dimension=0, tiled=True
    )
    pair = exchanged(pieces, "row_0").astype(jnp.float32)
    lowrank = pair[0] + pair[1]
    first_new = decay_first * first_moment + (1.0 - decay_first) * lowrank
    second_new = decay_second * second_moment + (1.0 - decay_second) * lowrank * lowrank
    direction = first_new / bias_first / (jnp.sqrt(second_new / bias_second) + epsilon)
    gathered = direction.astype(jnp.bfloat16)[None]
    for axis in ("row_0", "row_1"):
        gathered = lax.all_gather(gathered, axis, axis=0, tiled=True)
    total = by_axis(jnp.sum(direction * direction), ROW_COL)
    root_mean = jnp.sqrt(total / (R * FF) + 1e-06)
    factor = jnp.minimum(1.0, clip_limit / root_mean)
    basis = projector.reshape(-1, row_0, row_1, rows).swapaxes(1, 2).reshape(projector.shape)
    basis = lax.optimization_barrier(basis)
    projected = jnp.dot(
        basis, gathered.reshape(basis.shape[1], -1), preferred_element_type=jnp.float32
    )
    updates = (factor * projected).astype(jnp.bfloat16)
    return (updates, first_new, second_new)


def solution(mesh):
    torus = Mesh(
        mesh.devices.reshape(2, 16, 4, 2, 2), ("row_0", "row_1", "col_0", "col_1", "col_2")
    )
    in_specs = (P(ROW, COL), P(ROW, None), P(ROW, COL), P(ROW, COL))
    out_specs = (P(ROW, COL), P(ROW, COL), P(ROW, COL))
    return jax.shard_map(local, mesh=torus, in_specs=in_specs, out_specs=out_specs, check_vma=False)
```

```python
import jax
import jax.numpy as jnp
from jax import lax
from jax.sharding import Mesh
from jax.sharding import PartitionSpec as P

FF = 28672
R = 1024
LANES = 128
ROW = ("x_lo", "z_hi", "z_lo")
COL = ("y", "x_hi", "core")
SQUARE = ("x_lo", "z_lo")


decay_first = 0.9
decay_second = 0.999
bias_first = 1.0 - 0.9**10
bias_second = 1.0 - 0.999**10
epsilon = 1e-08
clip_limit = 0.5


def exchanged(pieces, axes):
    return lax.all_to_all(pieces, axes, split_axis=0, concat_axis=0, tiled=True)


def spread(block, axes):
    return exchanged(jnp.broadcast_to(block, (lax.axis_size(axes), *block.shape)), axes)


def column_blocks(array, parts, width):
    rows, columns = array.shape
    array = jnp.pad(array, ((0, 0), (0, parts * width - columns)))
    return array.reshape(rows, parts, width).swapaxes(0, 1)


def side_by_side(blocks, columns):
    return blocks.swapaxes(0, 1).reshape(blocks.shape[1], -1)[:, :columns]


def summed_everywhere(value):
    value = jnp.full((8, LANES), value, jnp.float32)
    for axes in (SQUARE, "z_hi", COL):
        value = jnp.sum(spread(value, axes), axis=0)
    return value[0, 0]


def local(gradient, projector, first_moment, second_moment):
    block_rows, columns = gradient.shape
    ranks = projector.shape[1]
    rows = first_moment.shape[0]
    square = lax.axis_size(SQUARE)
    z_hi, z_lo = lax.axis_size("z_hi"), lax.axis_size("z_lo")
    width = -(-columns // (square * LANES)) * LANES
    half = ranks // 2

    basis = projector.reshape(block_rows, -1, z_hi, z_lo * rows).swapaxes(1, 2)
    basis = basis.reshape(block_rows, ranks)
    own_half = lax.dynamic_slice_in_dim(basis, lax.axis_index("core") * half, half, 1)
    halves = spread(spread(own_half, SQUARE).reshape(square * block_rows, half), "core")

    block = exchanged(column_blocks(gradient, square, width), SQUARE)
    block = block.reshape(square * block_rows, width)
    partial = jnp.concatenate(
        [
            lax.dot_general(
                halves[k], block, (((0,), (0,)), ((), ())), preferred_element_type=jnp.float32
            ).astype(jnp.bfloat16)
            for k in range(2)
        ]
    )
    summed = lax.psum_scatter(
        partial.reshape(z_hi, ranks // z_hi, width), "z_hi", scatter_dimension=0, tiled=True
    )
    lowrank = exchanged(summed.reshape(square, rows, width), SQUARE)
    lowrank = side_by_side(lowrank, columns).astype(jnp.float32)

    first_new = decay_first * first_moment + (1.0 - decay_first) * lowrank
    second_new = decay_second * second_moment + (1.0 - decay_second) * lowrank * lowrank
    direction = first_new / bias_first / (jnp.sqrt(second_new / bias_second) + epsilon)

    step = exchanged(column_blocks(direction.astype(jnp.bfloat16), square, width), SQUARE)
    step = lax.all_gather(step.reshape(square * rows, width), "z_hi", axis=0, tiled=True)
    total = summed_everywhere(jnp.sum(direction * direction))
    root_mean = jnp.sqrt(total / (R * FF) + 1e-06)
    factor = jnp.minimum(1.0, clip_limit / root_mean)
    whole = lax.optimization_barrier(jnp.concatenate([halves[0], halves[1]], axis=1))
    projected = jnp.dot(whole, step, preferred_element_type=jnp.float32)
    updates = (factor * projected).astype(jnp.bfloat16)
    updates = exchanged(updates.reshape(square, block_rows, width), SQUARE)
    return (side_by_side(updates, columns), first_new, second_new)


def solution(mesh):
    torus = Mesh(mesh.devices.reshape(2, 8, 2, 4, 2, 2), (*ROW, *COL))
    in_specs = (P(ROW, COL), P(ROW, None), P(ROW, COL), P(ROW, COL))
    out_specs = (P(ROW, COL), P(ROW, COL), P(ROW, COL))
    return jax.shard_map(local, mesh=torus, in_specs=in_specs, out_specs=out_specs, check_vma=False)
```

```python
import jax
import jax.numpy as jnp
from jax import lax
from jax.sharding import Mesh
from jax.sharding import PartitionSpec as P

FF = 28672
R = 1024
LANES = 128
ROW = ("x_lo", "z_hi", "z_lo")
COL = ("y", "x_hi", "core")
SQUARE = ("x_lo", "z_lo")


decay_first = 0.9
decay_second = 0.999
bias_first = 1.0 - 0.9**10
bias_second = 1.0 - 0.999**10
epsilon = 1e-08
clip_limit = 0.5


def exchanged(pieces, axes):
    return lax.all_to_all(pieces, axes, split_axis=0, concat_axis=0, tiled=True)


def spread(block, axes):
    return exchanged(jnp.broadcast_to(block, (lax.axis_size(axes), *block.shape)), axes)


def column_blocks(array, parts, width):
    rows, columns = array.shape
    array = jnp.pad(array, ((0, 0), (0, parts * width - columns)))
    return array.reshape(rows, parts, width).swapaxes(0, 1)


def side_by_side(blocks, columns):
    return blocks.swapaxes(0, 1).reshape(blocks.shape[1], -1)[:, :columns]


def rank_order(basis, split, order):
    basis = basis.reshape(-1, *split).transpose(0, *(1 + axis for axis in order))
    return basis.reshape(basis.shape[0], -1)


def summed_everywhere(value):
    value = jnp.full((8, LANES), value, jnp.float32)
    for axes in (SQUARE, "z_hi", COL):
        value = jnp.sum(spread(value, axes), axis=0)
    return value[0, 0]


def local(gradient, projector, first_moment, second_moment):
    block_rows, columns = gradient.shape
    ranks = projector.shape[1]
    rows = first_moment.shape[0]
    square = lax.axis_size(SQUARE)
    x_lo, z_hi, z_lo = (lax.axis_size(a) for a in ROW)
    width = -(-columns // (square * LANES)) * LANES
    half = ranks // 2

    ordered = rank_order(projector, (x_lo, z_hi, z_lo, rows), (1, 2, 0, 3))
    partial = lax.dot_general(
        ordered, gradient, (((0,), (0,)), ((), ())), preferred_element_type=jnp.float32
    ).astype(jnp.bfloat16)
    partial, projector = lax.optimization_barrier((partial, projector))
    pieces = partial.reshape(z_hi * z_lo * x_lo, rows, columns)
    pieces = lax.psum_scatter(pieces, ("z_hi", "z_lo"), scatter_dimension=0, tiled=True)

    basis = rank_order(projector, (x_lo, z_hi, z_lo, rows), (1, 0, 2, 3))
    own_half = lax.dynamic_slice_in_dim(basis, lax.axis_index("core") * half, half, 1)
    halves = spread(spread(own_half, SQUARE).reshape(square * block_rows, half), "core")
    whole = jnp.concatenate([halves[0], halves[1]], axis=1)
    pieces, whole = lax.optimization_barrier((pieces, whole))

    pair = exchanged(pieces, "x_lo").astype(jnp.float32)
    lowrank = pair[0] + pair[1]
    first_new = decay_first * first_moment + (1.0 - decay_first) * lowrank
    second_new = decay_second * second_moment + (1.0 - decay_second) * lowrank * lowrank
    direction = first_new / bias_first / (jnp.sqrt(second_new / bias_second) + epsilon)

    step = exchanged(column_blocks(direction.astype(jnp.bfloat16), square, width), SQUARE)
    step = lax.all_gather(step.reshape(square * rows, width), "z_hi", axis=0, tiled=True)
    total = summed_everywhere(jnp.sum(direction * direction))
    root_mean = jnp.sqrt(total / (R * FF) + 1e-06)
    factor = jnp.minimum(1.0, clip_limit / root_mean)
    projected = jnp.dot(whole, step, preferred_element_type=jnp.float32)
    updates = (factor * projected).astype(jnp.bfloat16)
    updates = exchanged(updates.reshape(square, block_rows, width), SQUARE)
    return (side_by_side(updates, columns), first_new, second_new)


def solution(mesh):
    torus = Mesh(mesh.devices.reshape(2, 8, 2, 4, 2, 2), (*ROW, *COL))
    in_specs = (P(ROW, COL), P(ROW, None), P(ROW, COL), P(ROW, COL))
    out_specs = (P(ROW, COL), P(ROW, COL), P(ROW, COL))
    return jax.shard_map(local, mesh=torus, in_specs=in_specs, out_specs=out_specs, check_vma=False)
```

```python
import functools

import jax
import jax.numpy as jnp
from jax import lax
from jax.sharding import Mesh
from jax.sharding import PartitionSpec as P

FF = 28672
R = 1024
LANES = 128
ROW = ("x_lo", "z_hi", "z_lo")
COL = ("y", "x_hi", "core")
SQUARE = ("x_lo", "z_lo")


decay_first = 0.9
decay_second = 0.999
bias_first = 1.0 - 0.9**10
bias_second = 1.0 - 0.999**10
epsilon = 1e-08
clip_limit = 0.5


def exchanged(pieces, axes):
    return lax.all_to_all(pieces, axes, split_axis=0, concat_axis=0, tiled=True)


def spread(block, axes):
    return exchanged(jnp.broadcast_to(block, (lax.axis_size(axes), *block.shape)), axes)


def column_blocks(array, parts, width):
    rows, columns = array.shape
    array = jnp.pad(array, ((0, 0), (0, parts * width - columns)))
    return array.reshape(rows, parts, width).swapaxes(0, 1)


def side_by_side(blocks, columns):
    return blocks.swapaxes(0, 1).reshape(blocks.shape[1], -1)[:, :columns]


def adam(lowrank, first_moment, second_moment):
    first_new = decay_first * first_moment + (1.0 - decay_first) * lowrank
    second_new = decay_second * second_moment + (1.0 - decay_second) * lowrank * lowrank
    direction = first_new / bias_first / (jnp.sqrt(second_new / bias_second) + epsilon)
    return first_new, second_new, direction


def summed_everywhere(value):
    value = jnp.full((8, LANES), value, jnp.float32)
    for axes in (SQUARE, "z_hi", COL):
        value = jnp.sum(spread(value, axes), axis=0)
    return value[0, 0]


def local(gradient, projector, first_moment, second_moment):
    block_rows, columns = gradient.shape
    ranks = projector.shape[1]
    rows = first_moment.shape[0]
    square = lax.axis_size(SQUARE)
    x_lo, z_hi, z_lo = (lax.axis_size(a) for a in ROW)
    width = -(-columns // (square * LANES)) * LANES
    half = ranks // 2

    split = (ranks // (z_hi * z_lo * rows), z_hi * z_lo, rows)
    ordered = projector.reshape(block_rows, *split).swapaxes(1, 2).reshape(block_rows, ranks)
    partial = lax.dot_general(
        ordered, gradient, (((0,), (0,)), ((), ())), preferred_element_type=jnp.float32
    ).astype(jnp.bfloat16)
    partial, ordered, first_moment, second_moment = lax.optimization_barrier(
        (partial, ordered, first_moment, second_moment)
    )
    pieces = partial.reshape(z_hi * z_lo * x_lo, rows, columns)
    pieces = lax.psum_scatter(pieces, ("z_hi", "z_lo"), scatter_dimension=0, tiled=True)

    own_half = lax.dynamic_slice_in_dim(ordered, lax.axis_index("core") * half, half, 1)
    halves = spread(spread(own_half, SQUARE).reshape(square * block_rows, half), "core")
    whole = jnp.concatenate([halves[0], halves[1]], axis=1)
    moments = jnp.concatenate([first_moment, second_moment])
    moments = exchanged(column_blocks(moments, square, width), SQUARE)
    moments = moments.reshape(x_lo, z_lo, 2, rows, width).transpose(2, 1, 0, 3, 4)
    pieces, whole, moments = lax.optimization_barrier((pieces, whole, moments))

    quarter = exchanged(column_blocks(pieces.reshape(x_lo * rows, columns), square, width), SQUARE)
    quarter = quarter.reshape(x_lo, z_lo, x_lo, rows, width).astype(jnp.float32)
    quarter = functools.reduce(jnp.add, [quarter[k] for k in range(x_lo)])
    direction = adam(quarter, moments[0], moments[1])[2]
    step = direction.astype(jnp.bfloat16).reshape(square * rows, width)
    step, pieces = lax.optimization_barrier((step, pieces))
    step = lax.all_gather(step, "z_hi", axis=0, tiled=True)
    total = summed_everywhere(jnp.sum(direction * direction))

    pair = exchanged(pieces, "x_lo").astype(jnp.float32)
    first_new, second_new, _ = adam(
        functools.reduce(jnp.add, [pair[k] for k in range(x_lo)]), first_moment, second_moment
    )

    root_mean = jnp.sqrt(total / (R * FF) + 1e-06)
    factor = jnp.minimum(1.0, clip_limit / root_mean)
    projected = jnp.dot(whole, step, preferred_element_type=jnp.float32)
    updates = (factor * projected).astype(jnp.bfloat16)
    updates = exchanged(updates.reshape(square, block_rows, width), SQUARE)
    return (side_by_side(updates, columns), first_new, second_new)


def solution(mesh):
    torus = Mesh(mesh.devices.reshape(2, 8, 2, 4, 2, 2), (*ROW, *COL))
    in_specs = (P(ROW, COL), P(ROW, None), P(ROW, COL), P(ROW, COL))
    out_specs = (P(ROW, COL), P(ROW, COL), P(ROW, COL))
    return jax.shard_map(local, mesh=torus, in_specs=in_specs, out_specs=out_specs, check_vma=False)
```

```python
import jax
import jax.numpy as jnp
from jax import lax
from jax.sharding import Mesh
from jax.sharding import PartitionSpec as P

FF = 28672
R = 1024
LANES = 128
ROW = ("x_lo", "z_hi", "z_lo")
COL = ("y", "x_hi", "core")
SQUARE = ("x_lo", "z_lo")


decay_first = 0.9
decay_second = 0.999
bias_first = 1.0 - 0.9**10
bias_second = 1.0 - 0.999**10
epsilon = 1e-08
clip_limit = 0.5


def exchanged(pieces, axes):
    return lax.all_to_all(pieces, axes, split_axis=0, concat_axis=0, tiled=True)


def spread(block, axes):
    return exchanged(jnp.broadcast_to(block, (lax.axis_size(axes), *block.shape)), axes)


def column_blocks(array, parts, width):
    rows, columns = array.shape
    array = jnp.pad(array, ((0, 0), (0, parts * width - columns)))
    return array.reshape(rows, parts, width).swapaxes(0, 1)


def side_by_side(blocks, columns):
    return blocks.swapaxes(0, 1).reshape(blocks.shape[1], -1)[:, :columns]


def adam(lowrank, first_moment, second_moment):
    first_new = decay_first * first_moment + (1.0 - decay_first) * lowrank
    second_new = decay_second * second_moment + (1.0 - decay_second) * lowrank * lowrank
    direction = first_new / bias_first / (jnp.sqrt(second_new / bias_second) + epsilon)
    return first_new, second_new, direction


def summed_everywhere(value):
    value = jnp.full((8, LANES), value, jnp.float32)
    for axes in (SQUARE, "z_hi", COL):
        value = jnp.sum(spread(value, axes), axis=0)
    return value[0, 0]


def local(gradient, projector, first_moment, second_moment):
    block_rows, columns = gradient.shape
    ranks = projector.shape[1]
    rows = first_moment.shape[0]
    square = lax.axis_size(SQUARE)
    x_lo, z_hi, z_lo = (lax.axis_size(a) for a in ROW)
    width = -(-columns // (square * LANES)) * LANES
    half = ranks // 2
    core = lax.axis_index("core")

    def own_first(array, axis):
        return jnp.where(core == 0, array, jnp.flip(array, axis))

    ordered = projector.reshape(block_rows, x_lo, z_hi, z_lo, rows).transpose(0, 3, 2, 1, 4)
    own_half = lax.dynamic_slice_in_dim(ordered.reshape(block_rows, ranks), core * half, half, 1)
    own_half = spread(own_half, SQUARE).reshape(square * block_rows, half)
    blocks = column_blocks(gradient, square, width)
    own_half, blocks = lax.optimization_barrier((own_half, blocks))
    other_half = lax.ppermute(own_half, "core", [(0, 1), (1, 0)])
    block = exchanged(blocks, SQUARE).reshape(square * block_rows, width)
    partial = [
        lax.dot_general(
            basis, block, (((0,), (0,)), ((), ())), preferred_element_type=jnp.float32
        ).astype(jnp.bfloat16)
        for basis in (own_half, other_half)
    ]
    partial = jnp.stack([p.reshape(z_hi, half // z_hi, width) for p in partial], axis=1)
    partial = partial.reshape(z_hi, ranks // z_hi, width)
    partial, own_half, other_half, first_moment, second_moment = lax.optimization_barrier(
        (partial, own_half, other_half, first_moment, second_moment)
    )
    summed = lax.psum_scatter(partial, "z_hi", scatter_dimension=0, tiled=True)

    whole = jnp.stack(
        [basis.reshape(-1, z_hi, half // z_hi) for basis in (own_half, other_half)], axis=2
    ).reshape(square * block_rows, ranks)
    moments = jnp.concatenate([first_moment, second_moment])
    moments = exchanged(column_blocks(moments, square, width), SQUARE)
    moments = moments.reshape(x_lo, z_lo, 2, rows, width).transpose(2, 1, 0, 3, 4)
    moments = own_first(moments, 1).reshape(2, square * rows, width)
    summed, whole, moments = lax.optimization_barrier((summed, whole, moments))

    summed = summed.reshape(square * rows, width)
    direction = adam(summed.astype(jnp.float32), moments[0], moments[1])[2]
    step = direction.astype(jnp.bfloat16)
    step, summed = lax.optimization_barrier((step, summed))
    step = lax.all_gather(step, "z_hi", axis=0, tiled=True)
    total = summed_everywhere(jnp.sum(direction * direction))

    lowrank = own_first(summed.reshape(z_lo, x_lo, rows, width), 0).swapaxes(0, 1)
    lowrank = exchanged(lowrank.reshape(square, rows, width), SQUARE)
    lowrank = side_by_side(lowrank, columns).astype(jnp.float32)
    first_new, second_new, _ = adam(lowrank, first_moment, second_moment)

    root_mean = jnp.sqrt(total / (R * FF) + 1e-06)
    factor = jnp.minimum(1.0, clip_limit / root_mean)
    projected = jnp.dot(whole, step, preferred_element_type=jnp.float32)
    updates = (factor * projected).astype(jnp.bfloat16)
    updates = exchanged(updates.reshape(square, block_rows, width), SQUARE)
    return (side_by_side(updates, columns), first_new, second_new)


def solution(mesh):
    torus = Mesh(mesh.devices.reshape(2, 8, 2, 4, 2, 2), (*ROW, *COL))
    in_specs = (P(ROW, COL), P(ROW, None), P(ROW, COL), P(ROW, COL))
    out_specs = (P(ROW, COL), P(ROW, COL), P(ROW, COL))
    return jax.shard_map(local, mesh=torus, in_specs=in_specs, out_specs=out_specs, check_vma=False)
```

```python
import jax
import jax.numpy as jnp
from jax import lax
from jax.sharding import Mesh
from jax.sharding import PartitionSpec as P

FF = 28672
R = 1024
LANES = 128
ROW = ("x_lo", "z_hi", "z_lo")
COL = ("y", "x_hi", "core")
SQUARE = ("x_lo", "z_lo")


decay_first = 0.9
decay_second = 0.999
bias_first = 1.0 - 0.9**10
bias_second = 1.0 - 0.999**10
epsilon = 1e-08
clip_limit = 0.5


def exchanged(pieces, axes):
    return lax.all_to_all(pieces, axes, split_axis=0, concat_axis=0, tiled=True)


def spread(block, axes):
    return exchanged(jnp.broadcast_to(block, (lax.axis_size(axes), *block.shape)), axes)


def column_blocks(array, parts, width):
    rows, columns = array.shape
    array = jnp.pad(array, ((0, 0), (0, parts * width - columns)))
    return array.reshape(rows, parts, width).swapaxes(0, 1)


def side_by_side(blocks, columns):
    return blocks.swapaxes(0, 1).reshape(blocks.shape[1], -1)[:, :columns]


def adam(lowrank, first_moment, second_moment):
    first_new = decay_first * first_moment + (1.0 - decay_first) * lowrank
    second_new = decay_second * second_moment + (1.0 - decay_second) * lowrank * lowrank
    direction = first_new / bias_first / (jnp.sqrt(second_new / bias_second) + epsilon)
    return first_new, second_new, direction


def summed_everywhere(value):
    value = jnp.full((8, LANES), value, jnp.float32)
    for axes in (SQUARE, "z_hi", COL):
        value = jnp.sum(spread(value, axes), axis=0)
    return value[0, 0]


def local(gradient, projector, first_moment, second_moment):
    block_rows, columns = gradient.shape
    ranks = projector.shape[1]
    rows = first_moment.shape[0]
    square = lax.axis_size(SQUARE)
    x_lo, z_hi, z_lo = (lax.axis_size(a) for a in ROW)
    width = columns // square
    half = ranks // 2
    core = lax.axis_index("core")

    def own_first(array, axis):
        return jnp.where(core == 0, array, jnp.flip(array, axis))

    ordered = projector.reshape(block_rows, x_lo, z_hi, z_lo, rows).transpose(0, 3, 2, 1, 4)
    own_half = lax.dynamic_slice_in_dim(ordered.reshape(block_rows, ranks), core * half, half, 1)
    own_half = spread(own_half, SQUARE).reshape(square * block_rows, half)
    blocks = column_blocks(gradient, square, width)
    own_half, blocks = lax.optimization_barrier((own_half, blocks))
    other_half = lax.ppermute(own_half, "core", [(0, 1), (1, 0)])
    block = exchanged(blocks, SQUARE).reshape(square * block_rows, width)
    partial = [
        lax.dot_general(
            basis, block, (((0,), (0,)), ((), ())), preferred_element_type=jnp.float32
        ).astype(jnp.bfloat16)
        for basis in (own_half, other_half)
    ]
    partial = jnp.stack([p.reshape(z_hi, half // z_hi, width) for p in partial], axis=1)
    partial = partial.reshape(z_hi, ranks // z_hi, width)
    partial, own_half, other_half, first_moment, second_moment = lax.optimization_barrier(
        (partial, own_half, other_half, first_moment, second_moment)
    )
    summed = lax.psum_scatter(partial, "z_hi", scatter_dimension=0, tiled=True)

    whole = jnp.stack(
        [basis.reshape(-1, z_hi, half // z_hi) for basis in (own_half, other_half)], axis=2
    ).reshape(square * block_rows, ranks)
    moments = jnp.concatenate([first_moment, second_moment])
    moments = exchanged(column_blocks(moments, square, width), SQUARE)
    moments = moments.reshape(x_lo, z_lo, 2, rows, width).transpose(2, 1, 0, 3, 4)
    moments = own_first(moments, 1).reshape(2, square * rows, width)
    summed, whole, moments = lax.optimization_barrier((summed, whole, moments))

    summed = summed.reshape(square * rows, width)
    direction = adam(summed.astype(jnp.float32), moments[0], moments[1])[2]
    step = jnp.pad(direction.astype(jnp.bfloat16), ((0, 0), (0, -width % LANES)))
    step, summed, moments = lax.optimization_barrier((step, summed, moments))
    step = lax.all_gather(step, "z_hi", axis=0, tiled=True)
    direction = adam(summed.astype(jnp.float32), moments[0], moments[1])[2]
    total = summed_everywhere(jnp.sum(direction * direction))

    lowrank = own_first(summed.reshape(z_lo, x_lo, rows, width), 0).swapaxes(0, 1)
    lowrank = exchanged(lowrank.reshape(square, rows, width), SQUARE)
    lowrank = side_by_side(lowrank, columns).astype(jnp.float32)
    first_new, second_new, _ = adam(lowrank, first_moment, second_moment)

    root_mean = jnp.sqrt(total / (R * FF) + 1e-06)
    factor = jnp.minimum(1.0, clip_limit / root_mean)
    projected = jnp.dot(whole, step[:, :width], preferred_element_type=jnp.float32)
    updates = (factor * projected).astype(jnp.bfloat16)
    updates = exchanged(updates.reshape(square, block_rows, width), SQUARE)
    return (side_by_side(updates, columns), first_new, second_new)


def solution(mesh):
    torus = Mesh(mesh.devices.reshape(2, 8, 2, 4, 2, 2), (*ROW, *COL))
    in_specs = (P(ROW, COL), P(ROW, None), P(ROW, COL), P(ROW, COL))
    out_specs = (P(ROW, COL), P(ROW, COL), P(ROW, COL))
    return jax.shard_map(local, mesh=torus, in_specs=in_specs, out_specs=out_specs, check_vma=False)
```

```python
import jax
import jax.numpy as jnp
from jax import lax
from jax.experimental import pallas as pl
from jax.sharding import Mesh
from jax.sharding import PartitionSpec as P

FF = 28672
R = 1024
LANES = 128
ROW = ("x_lo", "z_hi", "z_lo")
COL = ("y", "x_hi", "core")
SQUARE = ("x_lo", "z_lo")


decay_first = 0.9
decay_second = 0.999
bias_first = 1.0 - 0.9**10
bias_second = 1.0 - 0.999**10
epsilon = 1e-08
clip_limit = 0.5


def exchanged(pieces, axes):
    return lax.all_to_all(pieces, axes, split_axis=0, concat_axis=0, tiled=True)


def spread(block, axes):
    return exchanged(jnp.broadcast_to(block, (lax.axis_size(axes), *block.shape)), axes)


def column_blocks(array, parts, width):
    rows, columns = array.shape
    array = jnp.pad(array, ((0, 0), (0, parts * width - columns)))
    return array.reshape(rows, parts, width).swapaxes(0, 1)


def side_by_side(blocks, columns):
    return blocks.swapaxes(0, 1).reshape(blocks.shape[1], -1)[:, :columns]


def adam(lowrank, first_moment, second_moment):
    first_new = decay_first * first_moment + (1.0 - decay_first) * lowrank
    second_new = decay_second * second_moment + (1.0 - decay_second) * lowrank * lowrank
    direction = first_new / bias_first / (jnp.sqrt(second_new / bias_second) + epsilon)
    return first_new, second_new, direction


def projected_sums(own_half, other_half, block, square, groups):
    depth, half = own_half.shape
    width = block.shape[1]
    count = half // groups

    def kernel(own_ref, other_ref, block_ref, out_ref):
        for place, ref in enumerate((own_ref, other_ref)):
            total = jnp.zeros((half, width), jnp.float32)
            for k in range(square):
                total += lax.dot_general(
                    ref[k], block_ref[k], (((1,), (1,)), ((), ())), preferred_element_type=jnp.float32
                )
            total = total.astype(jnp.bfloat16)
            for group in range(groups):
                out_ref[group, place * count : (place + 1) * count, :] = total[
                    group * count : (group + 1) * count, :
                ]

    def turned(array):
        return array.reshape(square, depth // square, -1).swapaxes(1, 2)

    return pl.pallas_call(
        kernel,
        out_shape=jax.ShapeDtypeStruct((groups, 2 * count, width), jnp.bfloat16),
        cost_estimate=pl.CostEstimate(
            flops=4 * depth * half * width,
            bytes_accessed=4 * depth * half + 2 * depth * width + 4 * half * width,
            transcendentals=0,
        ),
    )(turned(own_half), turned(other_half), turned(block))


def summed_everywhere(value):
    value = jnp.full((8, LANES), value, jnp.float32)
    for axes in (SQUARE, "z_hi", COL):
        value = jnp.sum(spread(value, axes), axis=0)
    return value[0, 0]


def local(gradient, projector, first_moment, second_moment):
    block_rows, columns = gradient.shape
    ranks = projector.shape[1]
    rows = first_moment.shape[0]
    square = lax.axis_size(SQUARE)
    x_lo, z_hi, z_lo = (lax.axis_size(a) for a in ROW)
    width = columns // square
    half = ranks // 2
    core = lax.axis_index("core")

    def own_first(array, axis):
        return jnp.where(core == 0, array, jnp.flip(array, axis))

    ordered = projector.reshape(block_rows, x_lo, z_hi, z_lo, rows).transpose(0, 3, 2, 1, 4)
    own_half = lax.dynamic_slice_in_dim(ordered.reshape(block_rows, ranks), core * half, half, 1)
    own_half = spread(own_half, SQUARE).reshape(square * block_rows, half)
    blocks = column_blocks(gradient, square, width)
    own_half, blocks = lax.optimization_barrier((own_half, blocks))
    other_half = lax.ppermute(own_half, "core", [(0, 1), (1, 0)])
    block = exchanged(blocks, SQUARE).reshape(square * block_rows, width)
    partial = projected_sums(own_half, other_half, block, square, z_hi)
    partial, own_half, other_half, first_moment, second_moment = lax.optimization_barrier(
        (partial, own_half, other_half, first_moment, second_moment)
    )
    summed = lax.psum_scatter(partial, "z_hi", scatter_dimension=0, tiled=True)

    whole = jnp.stack(
        [basis.reshape(-1, z_hi, half // z_hi) for basis in (own_half, other_half)], axis=2
    ).reshape(square * block_rows, ranks)
    moments = jnp.concatenate([first_moment, second_moment])
    moments = exchanged(column_blocks(moments, square, width), SQUARE)
    moments = moments.reshape(x_lo, z_lo, 2, rows, width).transpose(2, 1, 0, 3, 4)
    moments = own_first(moments, 1).reshape(2, square * rows, width)
    summed, whole, moments = lax.optimization_barrier((summed, whole, moments))

    summed = summed.reshape(square * rows, width)
    direction = adam(summed.astype(jnp.float32), moments[0], moments[1])[2]
    step = jnp.pad(direction.astype(jnp.bfloat16), ((0, 0), (0, -width % LANES)))
    step, summed, moments = lax.optimization_barrier((step, summed, moments))
    step = lax.all_gather(step, "z_hi", axis=0, tiled=True)
    direction = adam(summed.astype(jnp.float32), moments[0], moments[1])[2]
    total = summed_everywhere(jnp.sum(direction * direction))

    lowrank = own_first(summed.reshape(z_lo, x_lo, rows, width), 0).swapaxes(0, 1)
    lowrank = exchanged(lowrank.reshape(square, rows, width), SQUARE)
    lowrank = side_by_side(lowrank, columns).astype(jnp.float32)
    first_new, second_new, _ = adam(lowrank, first_moment, second_moment)

    root_mean = jnp.sqrt(total / (R * FF) + 1e-06)
    factor = jnp.minimum(1.0, clip_limit / root_mean)
    projected = jnp.dot(whole, step[:, :width], preferred_element_type=jnp.float32)
    updates = (factor * projected).astype(jnp.bfloat16)
    updates = exchanged(updates.reshape(square, block_rows, width), SQUARE)
    return (side_by_side(updates, columns), first_new, second_new)


def solution(mesh):
    torus = Mesh(mesh.devices.reshape(2, 8, 2, 4, 2, 2), (*ROW, *COL))
    in_specs = (P(ROW, COL), P(ROW, None), P(ROW, COL), P(ROW, COL))
    out_specs = (P(ROW, COL), P(ROW, COL), P(ROW, COL))
    return jax.shard_map(local, mesh=torus, in_specs=in_specs, out_specs=out_specs, check_vma=False)
```

```python
import jax
import jax.numpy as jnp
from jax import lax
from jax.experimental import pallas as pl
from jax.experimental.pallas import tpu as pltpu
from jax.sharding import Mesh
from jax.sharding import PartitionSpec as P

FF = 28672
R = 1024
LANES = 128
ROW = ("x_lo", "z_hi", "z_lo")
COL = ("y", "x_hi", "core")
SQUARE = ("x_lo", "z_lo")


decay_first = 0.9
decay_second = 0.999
bias_first = 1.0 - 0.9**10
bias_second = 1.0 - 0.999**10
epsilon = 1e-08
clip_limit = 0.5


def exchanged(pieces, axes):
    return lax.all_to_all(pieces, axes, split_axis=0, concat_axis=0, tiled=True)


def spread(block, axes):
    return exchanged(jnp.broadcast_to(block, (lax.axis_size(axes), *block.shape)), axes)


def column_blocks(array, parts, width):
    rows, columns = array.shape
    array = jnp.pad(array, ((0, 0), (0, parts * width - columns)))
    return array.reshape(rows, parts, width).swapaxes(0, 1)


def side_by_side(blocks, columns):
    return blocks.swapaxes(0, 1).reshape(blocks.shape[1], -1)[:, :columns]


def adam(lowrank, first_moment, second_moment):
    first_new = decay_first * first_moment + (1.0 - decay_first) * lowrank
    second_new = decay_second * second_moment + (1.0 - decay_second) * lowrank * lowrank
    direction = first_new / bias_first / (jnp.sqrt(second_new / bias_second) + epsilon)
    return first_new, second_new, direction


def projected_sums(own_half, other_half, block, square, groups):
    depth, half = own_half.shape
    width = block.shape[1]
    count = half // groups

    def kernel(own_ref, other_ref, block_ref, out_ref):
        for place, ref in enumerate((own_ref, other_ref)):
            total = jnp.zeros((half, width), jnp.float32)
            for k in range(square):
                total += lax.dot_general(
                    ref[k], block_ref[k], (((1,), (1,)), ((), ())), preferred_element_type=jnp.float32
                )
            total = total.astype(jnp.bfloat16)
            for group in range(groups):
                out_ref[group, place * count : (place + 1) * count, :] = total[
                    group * count : (group + 1) * count, :
                ]

    def turned(array):
        return array.reshape(square, depth // square, -1).swapaxes(1, 2)

    return pl.pallas_call(
        kernel,
        in_specs=[pl.BlockSpec(memory_space=pltpu.VMEM)] * 3,
        compiler_params=pltpu.CompilerParams(vmem_limit_bytes=24 * 1024 * 1024),
        out_shape=jax.ShapeDtypeStruct((groups, 2 * count, width), jnp.bfloat16),
        cost_estimate=pl.CostEstimate(
            flops=4 * depth * half * width,
            bytes_accessed=4 * depth * half + 2 * depth * width + 4 * half * width,
            transcendentals=0,
        ),
    )(turned(own_half), turned(other_half), turned(block))


def summed_everywhere(value):
    value = jnp.full((8, LANES), value, jnp.float32)
    for axes in (SQUARE, "z_hi", COL):
        value = jnp.sum(spread(value, axes), axis=0)
    return value[0, 0]


def local(gradient, projector, first_moment, second_moment):
    block_rows, columns = gradient.shape
    ranks = projector.shape[1]
    rows = first_moment.shape[0]
    square = lax.axis_size(SQUARE)
    x_lo, z_hi, z_lo = (lax.axis_size(a) for a in ROW)
    width = columns // square
    half = ranks // 2
    core = lax.axis_index("core")

    def own_first(array, axis):
        return jnp.where(core == 0, array, jnp.flip(array, axis))

    ordered = projector.reshape(block_rows, x_lo, z_hi, z_lo, rows).transpose(0, 3, 2, 1, 4)
    own_half = lax.dynamic_slice_in_dim(ordered.reshape(block_rows, ranks), core * half, half, 1)
    own_half = spread(own_half, SQUARE).reshape(square * block_rows, half)
    blocks = column_blocks(gradient, square, width)
    own_half, blocks = lax.optimization_barrier((own_half, blocks))
    other_half = lax.ppermute(own_half, "core", [(0, 1), (1, 0)])
    block = exchanged(blocks, SQUARE).reshape(square * block_rows, width)
    partial = projected_sums(own_half, other_half, block, square, z_hi)
    partial, own_half, other_half, first_moment, second_moment = lax.optimization_barrier(
        (partial, own_half, other_half, first_moment, second_moment)
    )
    summed = lax.psum_scatter(partial, "z_hi", scatter_dimension=0, tiled=True)

    whole = jnp.stack(
        [basis.reshape(-1, z_hi, half // z_hi) for basis in (own_half, other_half)], axis=2
    ).reshape(square * block_rows, ranks)
    moments = jnp.concatenate([first_moment, second_moment])
    moments = exchanged(column_blocks(moments, square, width), SQUARE)
    moments = moments.reshape(x_lo, z_lo, 2, rows, width).transpose(2, 1, 0, 3, 4)
    moments = own_first(moments, 1).reshape(2, square * rows, width)
    summed, whole, moments = lax.optimization_barrier((summed, whole, moments))

    summed = summed.reshape(square * rows, width)
    direction = adam(summed.astype(jnp.float32), moments[0], moments[1])[2]
    step = jnp.pad(direction.astype(jnp.bfloat16), ((0, 0), (0, -width % LANES)))
    step, summed, moments = lax.optimization_barrier((step, summed, moments))
    step = lax.all_gather(step, "z_hi", axis=0, tiled=True)
    direction = adam(summed.astype(jnp.float32), moments[0], moments[1])[2]
    total = summed_everywhere(jnp.sum(direction * direction))

    lowrank = own_first(summed.reshape(z_lo, x_lo, rows, width), 0).swapaxes(0, 1)
    lowrank = exchanged(lowrank.reshape(square, rows, width), SQUARE)
    lowrank = side_by_side(lowrank, columns).astype(jnp.float32)
    first_new, second_new, _ = adam(lowrank, first_moment, second_moment)

    root_mean = jnp.sqrt(total / (R * FF) + 1e-06)
    factor = jnp.minimum(1.0, clip_limit / root_mean)
    projected = jnp.dot(whole, step[:, :width], preferred_element_type=jnp.float32)
    updates = (factor * projected).astype(jnp.bfloat16)
    updates = exchanged(updates.reshape(square, block_rows, width), SQUARE)
    return (side_by_side(updates, columns), first_new, second_new)


def solution(mesh):
    torus = Mesh(mesh.devices.reshape(2, 8, 2, 4, 2, 2), (*ROW, *COL))
    in_specs = (P(ROW, COL), P(ROW, None), P(ROW, COL), P(ROW, COL))
    out_specs = (P(ROW, COL), P(ROW, COL), P(ROW, COL))
    return jax.shard_map(local, mesh=torus, in_specs=in_specs, out_specs=out_specs, check_vma=False)
```
